32 devices in a mesh: ta: 2 (over y), sa: 16 (over z, x, core).
Axes of the slice: x: 2, y: 2, z: 4, core: 2. Of those that a mesh axis runs over, the one named last changes fastest.
Arguments:
- series: float32 [256, 65536], P('sa', 'ta'), may hold values from -6 to 6
- index_series: float32 [16, 65536], P(None, 'ta'), may hold values from -6 to 6
- assign: int32 [256], replicated, may hold values from 0 to 15
Outputs:
- autocorr: float32 [256, 4096], P('sa', 'ta')
- crosscorr: float32 [256, 4096], P('sa', 'ta')
The draws below stay inside these ranges and needn't reach their ends.
Inputs may be any that keep to these rules, and one draw needn't show every extreme that they name: `assign`: each series names one index series.
All inputs are finite; a program needn't handle non-finite values.
Results may differ from the reference program's by a relative error of at most 0.000098.
Values sent between devices are 32-bit elements; how exact they have to be, the bound alone decides.
A program may use at most 128 MiB of HBM per device.

```python
import jax
import jax.numpy as jnp

NIDX = 16
TIME = 65536
LAGS = 4096
SERIES = 256


def set_ends(array, rng, smallest, largest):
    spot = [jax.random.randint(jax.random.fold_in(rng, axis), (), 0, length) for axis, length in enumerate(array.shape)]
    widest = array.shape.index(max(array.shape))
    next_to = spot[:widest] + [(spot[widest] + 1) % array.shape[widest]] + spot[widest + 1:]
    return array.at[tuple(spot)].set(smallest).at[tuple(next_to)].set(largest)


def block_scale(own_key, shape, pieces, low, high):
    level = 1.0
    for dim, blocks in pieces:
        steps = jax.random.uniform(jax.random.fold_in(jax.random.fold_in(own_key, 6), dim), (blocks,), jnp.float32, low / len(pieces), high / len(pieces))
        level = level * jnp.repeat(jnp.exp(steps), shape[dim] // blocks).reshape((-1,) + (1,) * (len(shape) - 1 - dim))
    return level


def noise(key, dims, deviation, reach, pieces=(), held_as=jnp.bfloat16):
    loudness = block_scale(key, dims, pieces, -0.22, 0.18) if pieces else 1.0
    values = jax.random.normal(key, dims, jnp.float32) * deviation * loudness
    return jnp.minimum(jnp.maximum(values, -reach), reach).astype(held_as)


def setup_inputs(seed: int = 0) -> dict:
    key_of = jax.random.split(jax.random.key(seed), 4)
    series = noise(key_of[0], (SERIES, TIME), 1.0, 6.0, ((0, 16), (1, 2)), jnp.float32)
    index_series = noise(key_of[1], (NIDX, TIME), 1.0, 6.0, ((1, 2),), jnp.float32)
    assign = set_ends(jax.random.randint(key_of[2], (SERIES,), 0, NIDX), jax.random.fold_in(key_of[2], 1), 0, NIDX - 1).astype(jnp.int32)
    return {"series": series, "index_series": index_series, "assign": assign}


def reference(series, index_series, assign):
    fft_len = 2 * TIME
    spectrum = jnp.fft.rfft(series, n=fft_len, axis=1)
    index_spec = jnp.fft.rfft(index_series, n=fft_len, axis=1)
    partner = index_spec[assign]
    power_spec = spectrum.real * spectrum.real + spectrum.imag * spectrum.imag
    cross_spec = jnp.conj(spectrum) * partner
    factor = 1.0 / jnp.sqrt(jnp.float32(TIME))
    autocorr = jnp.fft.irfft(power_spec, n=fft_len, axis=1)[:, :LAGS] * factor
    crosscorr = jnp.fft.irfft(cross_spec, n=fft_len, axis=1)[:, :LAGS] * factor
    return (autocorr.astype(jnp.float32), crosscorr.astype(jnp.float32))
```

```python
import functools
import math

import jax
import jax.numpy as jnp
from jax import lax
from jax.experimental import pallas as pl
from jax.experimental.pallas import tpu as pltpu
from jax.sharding import PartitionSpec as P

LAGS = 4096
LANE = 128
SUB = 8


def split(x):
    hi = x.astype(jnp.bfloat16).astype(jnp.float32)
    return hi, x - hi


def correlate(assign_ref, halo_ref, ser_ref, idx_ref, auto_ref, cross_ref, hi_ref, lo_ref):
    group, row = pl.program_id(0), pl.program_id(1)
    q_len = ser_ref.shape[1] // SUB
    m_len = halo_ref.shape[1] // SUB
    which = assign_ref[group * SUB + row]
    own = ser_ref[0, pl.ds(row, q_len, stride=SUB), :]
    halo = halo_ref[0, pl.ds(row, m_len, stride=SUB), :]
    partner = idx_ref[which // SUB, pl.ds(which % SUB, q_len, stride=SUB), :]
    own_hi, own_lo = split(own)
    halo_hi, halo_lo = split(halo)
    hi_ref[:m_len, :] = halo_hi
    hi_ref[m_len:, :] = own_hi
    lo_ref[:m_len, :] = halo_lo
    lo_ref[m_len:, :] = own_lo
    late_hi, late_lo = split(jnp.concatenate([own.T, partner.T], axis=0))
    late_hi, late_lo = late_hi.astype(jnp.bfloat16), late_lo.astype(jnp.bfloat16)
    left = jnp.concatenate([late_hi, late_lo, late_hi], axis=1)

    def window(ref, m):
        return ref[m_len - m : m_len - m + q_len, :].astype(jnp.bfloat16)

    late = lax.broadcasted_iota(jnp.int32, (2 * LANE, LANE), 0) % LANE
    lane = lax.broadcasted_iota(jnp.int32, (2 * LANE, LANE), 1)
    same = lane <= late
    source = (late - lane) % LANE
    previous = None
    for first in range(0, m_len + 1, 2):
        ms = [m for m in (first, first + 1) if m <= m_len]
        early_hi = jnp.concatenate([window(hi_ref, m) for m in ms], axis=1)
        early_lo = jnp.concatenate([window(lo_ref, m) for m in ms], axis=1)
        right = jnp.concatenate([early_hi, early_hi, early_lo], axis=0)
        product = jnp.dot(left, right, preferred_element_type=jnp.float32)
        for place, m in enumerate(ms):
            block = product[:, place * LANE : (place + 1) * LANE]
            if previous is not None:
                both = jnp.where(same, previous, block)
                both = jnp.take_along_axis(both, source, axis=1)
                j = m - 1
                auto_ref[0, pl.ds(j * SUB + row, 1), :] = jnp.sum(both[:LANE], axis=0, keepdims=True)
                cross_ref[0, pl.ds(j * SUB + row, 1), :] = jnp.sum(both[LANE:], axis=0, keepdims=True)
            previous = block


def tiles(x):
    rows, cols = x.shape
    x = x.reshape(rows // SUB, SUB, cols // LANE, LANE)
    return x.transpose(0, 2, 1, 3).reshape(rows // SUB, cols // LANE * SUB, LANE)


def untile(x):
    groups, depth, _ = x.shape
    x = x.reshape(groups, depth // SUB, SUB, LANE).transpose(0, 2, 1, 3)
    return x.reshape(groups * SUB, depth // SUB * LANE)


def body(series, index_series, assign):
    n_time = lax.axis_size("ta")
    time_idx = lax.axis_index("ta")
    ser_idx = lax.axis_index("sa")
    ser_dev, t_local = series.shape
    own = tiles(series)
    index = tiles(index_series)
    groups, depth, _ = own.shape
    m_rows = LAGS // LANE * SUB
    halo = lax.ppermute(own[:, depth - m_rows :], "ta", [(i, i + 1) for i in range(n_time - 1)])
    mine = lax.dynamic_slice_in_dim(assign, ser_idx * ser_dev, ser_dev, 0)
    out = jax.ShapeDtypeStruct((groups, m_rows, LANE), jnp.float32)
    auto, cross = pl.pallas_call(
        correlate,
        out_shape=(out, out),
        grid_spec=pltpu.PrefetchScalarGridSpec(
            num_scalar_prefetch=1,
            grid=(groups, SUB),
            in_specs=[
                pl.BlockSpec((1, m_rows, LANE), lambda g, r, a: (g, 0, 0)),
                pl.BlockSpec((1, depth, LANE), lambda g, r, a: (g, 0, 0)),
                pl.BlockSpec(index.shape, lambda g, r, a: (0, 0, 0)),
            ],
            out_specs=[pl.BlockSpec((1, m_rows, LANE), lambda g, r, a: (g, 0, 0))] * 2,
            scratch_shapes=[pltpu.VMEM(((depth + m_rows) // SUB, LANE), jnp.float32)] * 2,
        ),
    )(mine, halo, own, index)
    both = jnp.stack([auto, cross])
    part = m_rows // n_time
    total = lax.dynamic_slice_in_dim(both, time_idx * part, part, 2)
    for step in range(1, n_time):
        target = (time_idx + step) % n_time
        sent = lax.dynamic_slice_in_dim(both, target * part, part, 2)
        total = total + lax.ppermute(sent, "ta", [(i, (i + step) % n_time) for i in range(n_time)])
    total = total * (1.0 / math.sqrt(n_time * t_local))
    return untile(total[0]), untile(total[1])


def solution(mesh):
    return jax.shard_map(
        body,
        mesh=mesh,
        in_specs=(P("sa", "ta"), P(None, "ta"), P()),
        out_specs=(P("sa", "ta"), P("sa", "ta")),
        check_vma=False,
    )
```
